32 devices in a mesh: tmpl: 8 (over y, x, core), grid: 4 (over z).
Axes of the slice: x: 2, y: 2, z: 4, core: 2. Of those that a mesh axis runs over, the one named last changes fastest.
Arguments:
- spectrum: float32 [256, 64, 64, 128], P('tmpl', 'grid'), may hold values from -12 to 12
Outputs:
- best_scores: float32 [4, 64, 64, 64], P(None, 'grid', 'tmpl')
- coherence: float32 [64, 64, 64], P('grid', 'tmpl')
The draws below stay inside these ranges and needn't reach their ends.
All inputs are finite; a program needn't handle non-finite values.
Results may differ from the reference program's by a relative error of at most 0.0001.
Values sent between devices are 32-bit elements; how exact they have to be, the bound alone decides.
A program may use at most 128 MiB of HBM per device.

```python
import math
import jax
import jax.numpy as jnp
from jax import lax

NG = 64
TEMPLATES = 256
TOP = 4


def log_uniform(key, shape, low, high):
    return jnp.exp(jax.random.uniform(key, shape, jnp.float32, math.log(low), math.log(high)))


def draw_spectrum(key, part):
    streams = jax.random.split(jax.random.fold_in(key, 11), 8)
    shape = (TEMPLATES, NG, NG, 2 * NG)
    base = jnp.clip(0.125 * jax.random.normal(streams[0], shape, jnp.float32), -0.75, 0.75)
    factor = log_uniform(streams[1], (TEMPLATES, NG, 1, 1), 0.5, 2.0)
    offset = jax.random.normal(streams[3], (TEMPLATES, NG), jnp.float32)
    values = base * factor
    values = values.at[:, :, :, 0].add(offset[:, :, None])
    return jnp.clip(values, -12.0, 12.0)


def setup_inputs(seed: int = 0) -> dict:
    streams_of = jax.random.split(jax.random.key(seed), 2)
    spectrum = draw_spectrum(jax.random.fold_in(streams_of[1], 71), 0)
    return dict(spectrum=spectrum)


FLOOR = -1e+30
SPREAD_FLOOR = 0.25

def phase_table(length):
    order = jnp.arange(length, dtype=jnp.int32)
    turns = order[:, None] * order[None, :] % length
    angle = turns.astype(jnp.float32) * (2.0 * math.pi / length)
    return jnp.concatenate([jnp.cos(angle), -jnp.sin(angle)], axis=0)

def merge_top(former, latter):
    result = []
    for rank_out in range(len(former)):
        winner = jnp.maximum(former[rank_out], latter[rank_out])
        for rank_in in range(rank_out):
            winner = jnp.maximum(winner, jnp.minimum(former[rank_in], latter[rank_out - rank_in - 1]))
        result.append(winner)
    return tuple(result)

def reference(spectrum):
    table = phase_table(NG)
    cell_count = float(NG * NG * NG)

    def advance(carry, coeffs):
        leaders, running = carry
        score = jnp.dot(coeffs.reshape(NG * NG, 2 * NG), table, precision=lax.Precision.HIGHEST, preferred_element_type=jnp.float32).reshape(NG, NG, NG)
        average = jnp.sum(score) / cell_count
        centred = score - average
        spread = jnp.sum(centred * centred) / cell_count
        normed = centred / jnp.sqrt(spread + SPREAD_FLOOR)
        filler = jnp.full((NG, NG, NG), FLOOR, jnp.float32)
        single = (normed,) + tuple((filler for rank_in in range(TOP - 1)))
        return ((merge_top(leaders, single), running + normed), None)
    start = tuple((jnp.full((NG, NG, NG), FLOOR, jnp.float32) for rank_in in range(TOP)))
    (leaders, running), unused = lax.scan(advance, (start, jnp.zeros((NG, NG, NG), jnp.float32)), spectrum)
    return (jnp.stack(leaders, axis=0), running / math.sqrt(TEMPLATES))
```

```python
import functools
import math

import jax
import jax.numpy as jnp
from jax import lax
from jax.experimental import pallas as pl
from jax.experimental.pallas import tpu as pltpu
from jax.sharding import PartitionSpec as P

TOP = 4
KEPT = TOP + 1
SPREAD_FLOOR = 0.25
CHUNKS = 8
LAG = 6
STEP = 4
TILE = 8
MB = 256
MESH = pl.DeviceIdType.MESH


def fill_table(table):
    doubled = table.shape[0] // 2
    points = doubled // 2
    shape = (doubled, doubled)
    row = lax.broadcasted_iota(jnp.int32, shape, 0)
    lane = lax.broadcasted_iota(jnp.int32, shape, 1)
    turns = (row % points) * (lane % points) + (row // points) * (points // 4)
    turns = (turns + points // 2) % points - points // 2
    phase = jnp.cos(turns.astype(jnp.float32) * (2.0 * math.pi / points))
    lead = phase.astype(jnp.bfloat16).astype(jnp.float32)
    for side in range(2):
        inside = (lane // points) == side
        rows = pl.ds(side * doubled, doubled)
        table[rows, :doubled] = jnp.where(inside, lead, 0.0).astype(jnp.bfloat16)
        table[rows, doubled:] = jnp.where(inside, phase - lead, 0.0).astype(jnp.bfloat16)


def order_pair(former, latter):
    return jnp.maximum(former, latter), jnp.minimum(former, latter)


def order_four(values):
    a, b = order_pair(values[0], values[1])
    c, d = order_pair(values[2], values[3])
    a, c = order_pair(a, c)
    b, d = order_pair(b, d)
    b, c = order_pair(b, c)
    return [a, b, c, d]


def merge_four(former, latter):
    a, b, c, d = (jnp.maximum(former[i], latter[TOP - 1 - i]) for i in range(TOP))
    a, c = order_pair(a, c)
    b, d = order_pair(b, d)
    a, b = order_pair(a, b)
    c, d = order_pair(c, d)
    return [a, b, c, d]


def merge_groups(former, latter):
    return merge_four(former[:TOP], latter[:TOP]) + [former[TOP] + latter[TOP]]


def bits_of(chips):
    return chips.bit_length() - 1


def bit_order(chips, chunk):
    bits = bits_of(chips)
    return [(chunk + phase) % bits for phase in range(bits)]


def shuffled(chips, chunk, chip):
    place = 0
    for bit in bit_order(chips, chunk):
        place = place * 2 + (chip >> bit) % 2
    return place


def kernel(groups, slabs, parts, chunks, spectrum_ref, packed_ref, *scratch):
    local_tmpl, slab_rows, beta_rows, doubled = spectrum_ref.shape
    points = doubled // 2
    half = slab_rows // 2
    chips = groups // 2
    bits = bits_of(chips)
    piece = beta_rows // groups
    per_chunk = half // chunks
    cell_count = float(points * points * points)
    scratch = list(scratch)
    take = scratch.pop
    held, table, score, stats, sent, gathered, average, scale, leaders, sibling = (take(0) for _ in range(10))
    work = [take(0) for _ in range(max(bits, 1))]
    arrived = [take(0) for _ in range(bits)]
    held_sem, stats_send, stats_recv, pair_send, pair_recv, far_send, far_recv = scratch

    place = lax.axis_index("tmpl")
    slab = lax.axis_index("grid")
    chip, core = place // 2, place % 2

    def fetch(number):
        return pltpu.make_async_copy(
            spectrum_ref.at[pl.ds(number * STEP, STEP)],
            held.at[pl.ds(number * STEP, STEP)],
            held_sem.at[number],
        )

    for number in range(local_tmpl // STEP):
        fetch(number).start(priority=1)

    def own_bit(bit):
        return (chip // 2**bit) % 2

    partner = (2 * chip + 1 - core, slab)
    across = [(2 * (chip + 2**bit * (1 - 2 * own_bit(bit))) + core, slab) for bit in range(bits)]
    near = [(place, (slab + step) % slabs) for step in range(1, slabs)]
    barrier = pltpu.get_barrier_semaphore()
    for device in [partner] + across + near:
        pl.semaphore_signal(barrier, inc=1, device_id=device, device_id_type=MESH)

    fill_table(table)

    def transform(number, carry):
        fetch(number).wait()
        base = number * STEP
        lines = MB // beta_rows
        for index in range(STEP):
            plain = square = None
            for block in range(half // lines):
                leads, rests = [], []
                for side in range(2):
                    coeffs = held[base + index, pl.ds(side * half + block * lines, lines)].reshape(MB, doubled)
                    lead = coeffs.astype(jnp.bfloat16)
                    leads.append(lead)
                    rests.append((coeffs - lead.astype(jnp.float32)).astype(jnp.bfloat16))
                both = jnp.dot(jnp.concatenate(leads, axis=1), table[...], preferred_element_type=jnp.float32)
                value = both[:, :doubled] + both[:, doubled:] + jnp.dot(jnp.concatenate(rests, axis=1), table[:, :doubled], preferred_element_type=jnp.float32)
                score[base + index, pl.ds(block * lines, lines)] = value.reshape(lines, beta_rows, doubled)
                one = value.reshape(MB // 8, 8, doubled)
                p = jnp.sum(one, axis=0)
                q = jnp.sum(one * one, axis=0)
                plain = p if plain is None else plain + p
                square = q if square is None else square + q
            stats[0, pl.ds(base + index, 1)] = jnp.sum(plain, axis=0, keepdims=True)
            stats[1, pl.ds(base + index, 1)] = jnp.sum(square, axis=0, keepdims=True)
        return carry

    def slots(part):
        tiles = (parts[part + 1] - parts[part]) // TILE
        width = doubled // (2 * tiles)
        lane = lax.broadcasted_iota(jnp.int32, (TILE, doubled), 1)
        places = [(kind, tile) for tile in range(tiles) for kind in range(2)]
        return [
            (kind, parts[part] + tile * TILE, (lane >= index * width) & (lane < (index + 1) * width), width)
            for index, (kind, tile) in enumerate(places)
        ]

    def share_stats(part):
        return [
            pltpu.make_async_remote_copy(
                src_ref=sent.at[part],
                dst_ref=gathered.at[part, step],
                send_sem=stats_send.at[part, step],
                recv_sem=stats_recv.at[part, step],
                device_id=near[step],
                device_id_type=MESH,
            )
            for step in range(slabs - 1)
        ]

    def publish(part):
        message = jnp.zeros((TILE, doubled), jnp.float32)
        for kind, row, mask, _ in slots(part):
            total = jnp.sum(stats[kind, pl.ds(row, TILE)], axis=-1, keepdims=True)
            message = jnp.where(mask, total, message)
        sent[part] = message
        for copy in share_stats(part):
            copy.start()

    def settle(part):
        total = sent[part]
        for step, copy in enumerate(share_stats(part)):
            copy.wait_recv()
            total = total + gathered[part, step]
        mean = None
        for kind, row, mask, width in slots(part):
            value = jnp.sum(jnp.where(mask, total, 0.0), axis=-1, keepdims=True) * (1.0 / (width * cell_count))
            if kind == 0:
                mean = value
                continue
            factor = 1.0 / jnp.sqrt(value - mean * mean + SPREAD_FLOOR)
            average[pl.ds(row, TILE)] = jnp.broadcast_to(mean, (TILE, doubled))
            scale[pl.ds(row, TILE)] = jnp.broadcast_to(factor, (TILE, doubled))

    def leading(part, chunk):
        low, high = parts[part], parts[part + 1]

        def one_row(row, carry):
            line = chunk * per_chunk + row
            for pair in range(chips):
                window = pl.ds(pair * 2 * piece, 2 * piece)
                running = None
                for base in range(low, high, TOP):
                    values = []
                    for tmpl in range(base, base + TOP):
                        centred = score[tmpl, line, window] - average[pl.ds(tmpl, 1)]
                        values.append(centred * scale[pl.ds(tmpl, 1)])
                    summed = (values[0] + values[1]) + (values[2] + values[3])
                    fresh = order_four(values) + [summed]
                    running = fresh if running is None else merge_groups(running, fresh)
                for side in range(2):
                    rows = slice(side * piece, (side + 1) * piece)
                    mine = [value[rows] for value in running]
                    if part > 0:
                        former = [leaders[chunk, side, pair, rank, row] for rank in range(KEPT)]
                        mine = merge_groups(former, mine)
                    for rank in range(KEPT):
                        leaders[chunk, side, pair, rank, row] = mine[rank]
            return carry

        lax.fori_loop(0, per_chunk, one_row, 0)

    def exchange(chunk):
        return pltpu.make_async_remote_copy(
            src_ref=leaders.at[chunk, 1 - core],
            dst_ref=sibling.at[chunk],
            send_sem=pair_send.at[chunk],
            recv_sem=pair_recv.at[chunk],
            device_id=partner,
            device_id_type=MESH,
        )

    def halving(phase, chunk):
        bit = bit_order(chips, chunk)[phase]
        kept = chips >> (phase + 1)
        return pltpu.make_async_remote_copy(
            src_ref=work[phase].at[chunk, pl.ds((1 - own_bit(bit)) * kept, kept)],
            dst_ref=arrived[phase].at[chunk],
            send_sem=far_send.at[phase, chunk],
            recv_sem=far_recv.at[phase, chunk],
            device_id=across[bit],
            device_id_type=MESH,
        )

    def hand_on(phase, chunk, slot, values):
        if phase < bits:
            for rank in range(KEPT):
                work[phase][chunk, slot, rank] = values[rank]
            return
        values[TOP] = values[TOP] / math.sqrt(groups * local_tmpl)
        for rank in range(KEPT):
            packed_ref[rank, pl.ds(chunk * per_chunk, per_chunk)] = values[rank]

    def join_pair(chunk):
        exchange(chunk).wait_recv()
        for pair in range(chips):
            former = [leaders[chunk, core, pair, rank] for rank in range(KEPT)]
            latter = [sibling[chunk, pair, rank] for rank in range(KEPT)]
            hand_on(0, chunk, shuffled(chips, chunk, pair), merge_groups(former, latter))
        if bits:
            halving(0, chunk).start()

    def join_far(phase, chunk):
        halving(phase, chunk).wait_recv()
        kept = chips >> (phase + 1)
        mine = own_bit(bit_order(chips, chunk)[phase]) * kept
        for slot in range(kept):
            former = [work[phase][chunk, mine + slot, rank] for rank in range(KEPT)]
            latter = [arrived[phase][chunk, slot, rank] for rank in range(KEPT)]
            hand_on(phase + 1, chunk, slot, merge_groups(former, latter))
        if phase + 1 < bits:
            halving(phase + 1, chunk).start()

    count = len(parts) - 1
    for part in range(count):
        lax.fori_loop(parts[part] // STEP, parts[part + 1] // STEP, transform, 0)
        if part == 0:
            pl.semaphore_wait(barrier, 1 + len(across) + len(near))
        publish(part)
    for part in range(count - 1):
        settle(part)
        for chunk in range(chunks):
            leading(part, chunk)
    settle(count - 1)
    for chunk in range(chunks):
        leading(count - 1, chunk)
        exchange(chunk).start()
        if chunk >= LAG:
            join_pair(chunk - LAG)
    for chunk in range(max(chunks - LAG, 0), chunks):
        join_pair(chunk)
    for phase in range(bits):
        for chunk in range(chunks):
            join_far(phase, chunk)
    for part in range(count):
        for copy in share_stats(part):
            copy.wait_send()
    for chunk in range(chunks):
        exchange(chunk).wait_send()
        for phase in range(bits):
            halving(phase, chunk).wait_send()


def unpack(packed_ref, best_ref, coherence_ref):
    half, points = packed_ref.shape[1], best_ref.shape[-1]
    for side in range(2):
        rows = pl.ds(side * half, half)
        lanes = slice(side * points, (side + 1) * points)
        best_ref[:, rows] = packed_ref[:TOP, :, :, lanes]
        coherence_ref[rows] = packed_ref[TOP, :, :, lanes]


def body(groups, slabs, spectrum):
    local_tmpl, slab_rows, beta_rows, doubled = spectrum.shape
    points = doubled // 2
    half = slab_rows // 2
    chips = groups // 2
    bits = bits_of(chips)
    piece = beta_rows // groups
    chunks = min(CHUNKS, half)
    per_chunk = half // chunks
    parts = (0, local_tmpl // 4 * 3, local_tmpl)
    count = len(parts) - 1
    block = (KEPT, per_chunk, piece, doubled)
    f32 = jnp.float32
    dma = pltpu.SemaphoreType.DMA
    packed = pl.pallas_call(
        functools.partial(kernel, groups, slabs, parts, chunks),
        out_shape=jax.ShapeDtypeStruct((KEPT, half, piece, doubled), f32),
        in_specs=[pl.BlockSpec(memory_space=pltpu.HBM)],
        out_specs=pl.BlockSpec(memory_space=pltpu.VMEM),
        scratch_shapes=[
            pltpu.VMEM((local_tmpl, slab_rows, beta_rows, doubled), f32),
            pltpu.VMEM((2 * doubled, 2 * doubled), jnp.bfloat16),
            pltpu.VMEM((local_tmpl, half, beta_rows, doubled), f32),
            pltpu.VMEM((2, local_tmpl, doubled), f32),
            pltpu.VMEM((count, TILE, doubled), f32),
            pltpu.VMEM((count, slabs - 1, TILE, doubled), f32),
            pltpu.VMEM((local_tmpl, doubled), f32),
            pltpu.VMEM((local_tmpl, doubled), f32),
            pltpu.VMEM((chunks, 2, chips) + block, f32),
            pltpu.VMEM((chunks, chips) + block, f32),
        ]
        + [pltpu.VMEM((chunks, chips >> phase) + block, f32) for phase in range(max(bits, 1))]
        + [pltpu.VMEM((chunks, chips >> (phase + 1)) + block, f32) for phase in range(bits)]
        + [
            dma((local_tmpl // STEP,)),
            dma((count, slabs - 1)),
            dma((count, slabs - 1)),
            dma((chunks,)),
            dma((chunks,)),
            dma((max(bits, 1), chunks)),
            dma((max(bits, 1), chunks)),
        ],
        compiler_params=pltpu.CompilerParams(
            collective_id=0, has_side_effects=True, vmem_limit_bytes=48 * 1024 * 1024
        ),
    )(spectrum)
    return pl.pallas_call(
        unpack,
        out_shape=(
            jax.ShapeDtypeStruct((TOP, slab_rows, piece, points), f32),
            jax.ShapeDtypeStruct((slab_rows, piece, points), f32),
        ),
        compiler_params=pltpu.CompilerParams(vmem_limit_bytes=8 * 1024 * 1024),
    )(packed)


def solution(mesh):
    return jax.shard_map(
        functools.partial(body, mesh.shape["tmpl"], mesh.shape["grid"]),
        mesh=mesh,
        in_specs=(P("tmpl", "grid", None, None),),
        out_specs=(P(None, "grid", "tmpl", None), P("grid", "tmpl", None)),
        check_vma=False,
    )
```

```python
import functools
import math

import jax
import jax.numpy as jnp
from jax import lax
from jax.experimental import pallas as pl
from jax.experimental.pallas import tpu as pltpu
from jax.sharding import PartitionSpec as P

TOP = 4
KEPT = TOP + 1
SPREAD_FLOOR = 0.25
CHUNKS = 8
HALVED = 4
STEP = 4
TILE = 8
MB = 256
MESH = pl.DeviceIdType.MESH


def fill_table(table):
    doubled = table.shape[0] // 2
    points = doubled // 2
    shape = (doubled, doubled)
    row = lax.broadcasted_iota(jnp.int32, shape, 0)
    lane = lax.broadcasted_iota(jnp.int32, shape, 1)
    turns = (row % points) * (lane % points) + (row // points) * (points // 4)
    turns = (turns + points // 2) % points - points // 2
    phase = jnp.cos(turns.astype(jnp.float32) * (2.0 * math.pi / points))
    lead = phase.astype(jnp.bfloat16).astype(jnp.float32)
    for side in range(2):
        inside = (lane // points) == side
        rows = pl.ds(side * doubled, doubled)
        table[rows, :doubled] = jnp.where(inside, lead, 0.0).astype(jnp.bfloat16)
        table[rows, doubled:] = jnp.where(inside, phase - lead, 0.0).astype(jnp.bfloat16)


def order_pair(former, latter):
    return jnp.maximum(former, latter), jnp.minimum(former, latter)


def order_four(values):
    a, b = order_pair(values[0], values[1])
    c, d = order_pair(values[2], values[3])
    a, c = order_pair(a, c)
    b, d = order_pair(b, d)
    b, c = order_pair(b, c)
    return [a, b, c, d]


def merge_four(former, latter):
    a, b, c, d = (jnp.maximum(former[i], latter[TOP - 1 - i]) for i in range(TOP))
    a, c = order_pair(a, c)
    b, d = order_pair(b, d)
    a, b = order_pair(a, b)
    c, d = order_pair(c, d)
    return [a, b, c, d]


def merge_groups(former, latter):
    return merge_four(former[:TOP], latter[:TOP]) + [former[TOP] + latter[TOP]]


def bits_of(chips):
    return chips.bit_length() - 1


def bit_order(chips, chunk):
    bits = bits_of(chips)
    return [(chunk + phase) % bits for phase in range(bits)]


def shuffled(chips, chunk, chip):
    place = 0
    for bit in bit_order(chips, chunk):
        place = place * 2 + (chip >> bit) % 2
    return place


def kernel(groups, slabs, parts, chunks, spectrum_ref, packed_ref, *scratch):
    local_tmpl, slab_rows, beta_rows, doubled = spectrum_ref.shape
    points = doubled // 2
    half = slab_rows // 2
    chips = groups // 2
    bits = bits_of(chips)
    piece = beta_rows // groups
    per_chunk = half // chunks
    cell_count = float(points * points * points)
    scratch = list(scratch)
    take = scratch.pop
    held, table, score, stats, sent, gathered, average, scale, leaders, sibling, extra, told = (take(0) for _ in range(12))
    work = [take(0) for _ in range(max(bits, 1))]
    arrived = [take(0) for _ in range(bits)]
    landed = take(0)
    halved = min(HALVED, chunks // 2)
    (
        held_sem, stats_send, stats_recv, told_send, told_recv, raw_send, raw_recv,
        pair_send, pair_recv, half_send, half_recv, far_send, far_recv,
    ) = scratch
    count = len(parts) - 1
    late = parts[count - 1]
    late_size = local_tmpl - late
    aligned = piece % TILE == 0

    place = lax.axis_index("tmpl")
    slab = lax.axis_index("grid")
    chip, core = place // 2, place % 2

    def fetch(number):
        return pltpu.make_async_copy(
            spectrum_ref.at[pl.ds(number * STEP, STEP)],
            held.at[pl.ds(number * STEP, STEP)],
            held_sem.at[number],
        )

    for number in range(local_tmpl // STEP):
        fetch(number).start(priority=1)

    def own_bit(bit):
        return (chip // 2**bit) % 2

    partner = (2 * chip + 1 - core, slab)
    across = [(2 * (chip + 2**bit * (1 - 2 * own_bit(bit))) + core, slab) for bit in range(bits)]
    far = [(2 * ((chip + step) % chips) + core, slab) for step in range(1, chips)]
    near = [(place, (slab + step) % slabs) for step in range(1, slabs)]
    beside = [(2 * chip + 1 - core, (slab + step) % slabs) for step in range(slabs)]
    barrier = pltpu.get_barrier_semaphore()
    for device in far + near + beside:
        pl.semaphore_signal(barrier, inc=1, device_id=device, device_id_type=MESH)

    fill_table(table)

    def transform(number, carry):
        fetch(number).wait()
        base = number * STEP
        lines = MB // beta_rows
        for index in range(STEP):
            plain = square = None
            for block in range(half // lines):
                leads, rests = [], []
                for side in range(2):
                    coeffs = held[base + index, pl.ds(side * half + block * lines, lines)].reshape(MB, doubled)
                    lead = coeffs.astype(jnp.bfloat16)
                    leads.append(lead)
                    rests.append((coeffs - lead.astype(jnp.float32)).astype(jnp.bfloat16))
                both = jnp.dot(jnp.concatenate(leads, axis=1), table[...], preferred_element_type=jnp.float32)
                value = both[:, :doubled] + both[:, doubled:] + jnp.dot(jnp.concatenate(rests, axis=1), table[:, :doubled], preferred_element_type=jnp.float32)
                score[base + index, pl.ds(block * lines, lines)] = value.reshape(lines, beta_rows, doubled)
                one = value.reshape(MB // 8, 8, doubled)
                p = jnp.sum(one, axis=0)
                q = jnp.sum(one * one, axis=0)
                plain = p if plain is None else plain + p
                square = q if square is None else square + q
            stats[0, pl.ds(base + index, 1)] = jnp.sum(plain, axis=0, keepdims=True)
            stats[1, pl.ds(base + index, 1)] = jnp.sum(square, axis=0, keepdims=True)
        return carry

    def slots(part):
        tiles = (parts[part + 1] - parts[part]) // TILE
        width = doubled // (2 * tiles)
        lane = lax.broadcasted_iota(jnp.int32, (TILE, doubled), 1)
        places = [(kind, tile) for tile in range(tiles) for kind in range(2)]
        return [
            (kind, parts[part] + tile * TILE, (lane >= index * width) & (lane < (index + 1) * width), width)
            for index, (kind, tile) in enumerate(places)
        ]

    def share_stats(part):
        return [
            pltpu.make_async_remote_copy(
                src_ref=sent.at[part],
                dst_ref=gathered.at[part, step],
                send_sem=stats_send.at[part, step],
                recv_sem=stats_recv.at[part, step],
                device_id=near[step],
                device_id_type=MESH,
            )
            for step in range(slabs - 1)
        ]

    def publish(part):
        message = jnp.zeros((TILE, doubled), jnp.float32)
        for kind, row, mask, _ in slots(part):
            total = jnp.sum(stats[kind, pl.ds(row, TILE)], axis=-1, keepdims=True)
            message = jnp.where(mask, total, message)
        sent[part] = message
        for copy in share_stats(part):
            copy.start()

    def tell_late():
        return [
            pltpu.make_async_remote_copy(
                src_ref=sent.at[count - 1],
                dst_ref=told.at[step],
                send_sem=told_send.at[step],
                recv_sem=told_recv.at[step],
                device_id=beside[step],
                device_id_type=MESH,
            )
            for step in range(slabs)
        ]

    def raw(number, owner):
        base = number * STEP
        spans = [(pair * 2 * piece + owner * piece, piece) for pair in range(chips)] if aligned else [(0, beta_rows)]
        return [
            pltpu.make_async_remote_copy(
                src_ref=score.at[pl.ds(base, STEP), :, pl.ds(pl.multiple_of(start, TILE), size)],
                dst_ref=extra.at[pl.ds(base - late, STEP), :, pl.ds(pl.multiple_of(start, TILE), size)],
                send_sem=raw_send.at[number - late // STEP, index],
                recv_sem=raw_recv.at[number - late // STEP, index],
                device_id=partner,
                device_id_type=MESH,
            )
            for index, (start, size) in enumerate(spans)
        ]

    def spread_out(part, total, shift):
        mean = None
        for kind, row, mask, width in slots(part):
            value = jnp.sum(jnp.where(mask, total, 0.0), axis=-1, keepdims=True) * (1.0 / (width * cell_count))
            if kind == 0:
                mean = value
                continue
            factor = 1.0 / jnp.sqrt(value - mean * mean + SPREAD_FLOOR)
            average[pl.ds(row + shift, TILE)] = jnp.broadcast_to(mean, (TILE, doubled))
            scale[pl.ds(row + shift, TILE)] = jnp.broadcast_to(factor, (TILE, doubled))

    def settle(part):
        for copy in share_stats(part):
            copy.wait_recv()
        if part == count - 1:
            for copy in tell_late():
                copy.wait_recv()
        total = sent[part]
        for step in range(slabs - 1):
            total = total + gathered[part, step]
        if part == count - 1:
            spread_out(part, sum((told[step] for step in range(1, slabs)), told[0]), late_size)
        spread_out(part, total, 0)

    def gather_up(running, values):
        summed = (values[0] + values[1]) + (values[2] + values[3])
        fresh = order_four(values) + [summed]
        return fresh if running is None else merge_groups(running, fresh)

    def last_leading(chunk):
        for row in range(per_chunk):
            line = chunk * per_chunk + row
            for pair in range(chips):
                start = pl.multiple_of(pair * 2 * piece + core * piece, piece)
                window = pl.ds(start, piece)
                running = None
                for base in range(late, local_tmpl, TOP):
                    running = gather_up(running, [
                        (score[tmpl, line, window] - average[pl.ds(tmpl, 1)]) * scale[pl.ds(tmpl, 1)]
                        for tmpl in range(base, base + TOP)
                    ])
                for base in range(0, late_size, TOP):
                    running = gather_up(running, [
                        (extra[tmpl, line, window] - average[pl.ds(local_tmpl + tmpl, 1)]) * scale[pl.ds(local_tmpl + tmpl, 1)]
                        for tmpl in range(base, base + TOP)
                    ])
                former = [leaders[chunk, core, pair, rank, row] for rank in range(KEPT)]
                latter = [sibling[chunk, pair, rank, row] for rank in range(KEPT)]
                running = merge_groups(running, merge_groups(former, latter))
                slot = shuffled(chips, chunk, pair) if chunk < halved else pair
                for rank in range(KEPT):
                    work[0][chunk, slot, rank, row] = running[rank]
        for copy in [halving(0, chunk)] if chunk < halved else scatter(chunk):
            copy.start()

    def leading(part, chunk):
        low, high = parts[part], parts[part + 1]

        def one_row(row, carry):
            line = chunk * per_chunk + row
            for pair in range(chips):
                window = pl.ds(pair * 2 * piece, 2 * piece)
                running = None
                for base in range(low, high, TOP):
                    running = gather_up(running, [
                        (score[tmpl, line, window] - average[pl.ds(tmpl, 1)]) * scale[pl.ds(tmpl, 1)]
                        for tmpl in range(base, base + TOP)
                    ])
                for side in range(2):
                    rows = slice(side * piece, (side + 1) * piece)
                    mine = [value[rows] for value in running]
                    if part > 0:
                        former = [leaders[chunk, side, pair, rank, row] for rank in range(KEPT)]
                        mine = merge_groups(former, mine)
                    for rank in range(KEPT):
                        leaders[chunk, side, pair, rank, row] = mine[rank]
            return carry

        lax.fori_loop(0, per_chunk, one_row, 0)

    def exchange(chunk):
        return pltpu.make_async_remote_copy(
            src_ref=leaders.at[chunk, 1 - core],
            dst_ref=sibling.at[chunk],
            send_sem=pair_send.at[chunk],
            recv_sem=pair_recv.at[chunk],
            device_id=partner,
            device_id_type=MESH,
        )

    def halving(phase, chunk):
        bit = bit_order(chips, chunk)[phase]
        kept = chips >> (phase + 1)
        return pltpu.make_async_remote_copy(
            src_ref=work[phase].at[chunk, pl.ds((1 - own_bit(bit)) * kept, kept)],
            dst_ref=arrived[phase].at[chunk],
            send_sem=half_send.at[phase, chunk],
            recv_sem=half_recv.at[phase, chunk],
            device_id=across[bit],
            device_id_type=MESH,
        )

    def scatter(chunk):
        return [
            pltpu.make_async_remote_copy(
                src_ref=work[0].at[chunk, (chip + step) % chips],
                dst_ref=landed.at[chunk - halved, step - 1],
                send_sem=far_send.at[chunk - halved, step - 1],
                recv_sem=far_recv.at[chunk - halved, step - 1],
                device_id=far[step - 1],
                device_id_type=MESH,
            )
            for step in range(1, chips)
        ]

    def join_scattered(chunk):
        for copy in scatter(chunk):
            copy.wait_recv()
        for row in range(per_chunk):
            running = [work[0][chunk, chip, rank, row] for rank in range(KEPT)]
            for step in range(chips - 1):
                running = merge_groups(running, [landed[chunk - halved, step, rank, row] for rank in range(KEPT)])
            hand_on(bits, chunk, 0, running, row)

    def hand_on(phase, chunk, slot, values, row):
        if phase < bits:
            for rank in range(KEPT):
                work[phase][chunk, slot, rank, row] = values[rank]
            return
        values[TOP] = values[TOP] / math.sqrt(groups * local_tmpl)
        for rank in range(KEPT):
            packed_ref[rank, chunk * per_chunk + row] = values[rank]

    def join_far(phase, chunk):
        halving(phase, chunk).wait_recv()
        kept = chips >> (phase + 1)
        mine = own_bit(bit_order(chips, chunk)[phase]) * kept
        for slot in range(kept):
            for row in range(per_chunk):
                former = [work[phase][chunk, mine + slot, rank, row] for rank in range(KEPT)]
                latter = [arrived[phase][chunk, slot, rank, row] for rank in range(KEPT)]
                hand_on(phase + 1, chunk, slot, merge_groups(former, latter), row)
        if phase + 1 < bits:
            halving(phase + 1, chunk).start()

    late_numbers = range(late // STEP, local_tmpl // STEP)
    for part in range(count - 1):
        lax.fori_loop(parts[part] // STEP, parts[part + 1] // STEP, transform, 0)
        if part == 0:
            pl.semaphore_wait(barrier, len(far) + len(near) + len(beside))
        publish(part)
    for number in late_numbers:
        transform(number, 0)
        if number == late_numbers[-1]:
            publish(count - 1)
            for copy in tell_late():
                copy.start()
        for copy in raw(number, 1 - core):
            copy.start()
    for part in range(count - 1):
        settle(part)
        for chunk in range(chunks):
            leading(part, chunk)
            if part == count - 2:
                exchange(chunk).start()
    for number in late_numbers:
        for copy in raw(number, core):
            copy.wait_recv()
    for chunk in range(chunks):
        exchange(chunk).wait_recv()
    settle(count - 1)
    for chunk in range(chunks):
        last_leading(chunk)
    for part in range(count):
        for copy in share_stats(part):
            copy.wait_send()
    for copy in tell_late():
        copy.wait_send()
    for number in late_numbers:
        for copy in raw(number, 1 - core):
            copy.wait_send()
    for chunk in range(chunks):
        exchange(chunk).wait_send()
    for chunk in range(halved):
        join_far(0, chunk)
    for chunk in range(halved):
        halving(0, chunk).wait_send()
    for chunk in range(halved, chunks):
        join_scattered(chunk)
    for phase in range(1, bits):
        for chunk in range(halved):
            join_far(phase, chunk)
    for chunk in range(halved, chunks):
        for copy in scatter(chunk):
            copy.wait_send()
    for phase in range(1, bits):
        for chunk in range(halved):
            halving(phase, chunk).wait_send()


def unpack(packed_ref, best_ref, coherence_ref):
    half, points = packed_ref.shape[1], best_ref.shape[-1]
    for side in range(2):
        rows = pl.ds(side * half, half)
        lanes = slice(side * points, (side + 1) * points)
        best_ref[:, rows] = packed_ref[:TOP, :, :, lanes]
        coherence_ref[rows] = packed_ref[TOP, :, :, lanes]


def body(groups, slabs, spectrum):
    local_tmpl, slab_rows, beta_rows, doubled = spectrum.shape
    points = doubled // 2
    half = slab_rows // 2
    chips = groups // 2
    bits = bits_of(chips)
    piece = beta_rows // groups
    chunks = min(CHUNKS, half)
    halved = min(HALVED, chunks // 2)
    per_chunk = half // chunks
    parts = (0, local_tmpl // 2, local_tmpl)
    late_size = parts[-1] - parts[-2]
    spans = chips if piece % TILE == 0 else 1
    count = len(parts) - 1
    block = (KEPT, per_chunk, piece, doubled)
    f32 = jnp.float32
    dma = pltpu.SemaphoreType.DMA
    packed = pl.pallas_call(
        functools.partial(kernel, groups, slabs, parts, chunks),
        out_shape=jax.ShapeDtypeStruct((KEPT, half, piece, doubled), f32),
        in_specs=[pl.BlockSpec(memory_space=pltpu.HBM)],
        out_specs=pl.BlockSpec(memory_space=pltpu.VMEM),
        scratch_shapes=[
            pltpu.VMEM((local_tmpl, slab_rows, beta_rows, doubled), f32),
            pltpu.VMEM((2 * doubled, 2 * doubled), jnp.bfloat16),
            pltpu.VMEM((local_tmpl, half, beta_rows, doubled), f32),
            pltpu.VMEM((2, local_tmpl, doubled), f32),
            pltpu.VMEM((count, TILE, doubled), f32),
            pltpu.VMEM((count, slabs - 1, TILE, doubled), f32),
            pltpu.VMEM((local_tmpl + late_size, doubled), f32),
            pltpu.VMEM((local_tmpl + late_size, doubled), f32),
            pltpu.VMEM((chunks, 2, chips) + block, f32),
            pltpu.VMEM((chunks, chips) + block, f32),
            pltpu.VMEM((late_size, half, beta_rows, doubled), f32),
            pltpu.VMEM((slabs, TILE, doubled), f32),
        ]
        + [pltpu.VMEM((chunks, chips >> phase) + block, f32) for phase in range(max(bits, 1))]
        + [pltpu.VMEM((chunks, chips >> (phase + 1)) + block, f32) for phase in range(bits)]
        + [pltpu.VMEM((chunks - halved, chips - 1) + block, f32)]
        + [
            dma((local_tmpl // STEP,)),
            dma((count, slabs - 1)),
            dma((count, slabs - 1)),
            dma((slabs,)),
            dma((slabs,)),
            dma((late_size // STEP, spans)),
            dma((late_size // STEP, spans)),
            dma((chunks,)),
            dma((chunks,)),
            dma((bits, chunks)),
            dma((bits, chunks)),
            dma((chunks - halved, chips - 1)),
            dma((chunks - halved, chips - 1)),
        ],
        compiler_params=pltpu.CompilerParams(
            collective_id=0, has_side_effects=True, vmem_limit_bytes=48 * 1024 * 1024
        ),
    )(spectrum)
    return pl.pallas_call(
        unpack,
        out_shape=(
            jax.ShapeDtypeStruct((TOP, slab_rows, piece, points), f32),
            jax.ShapeDtypeStruct((slab_rows, piece, points), f32),
        ),
        compiler_params=pltpu.CompilerParams(vmem_limit_bytes=8 * 1024 * 1024),
    )(packed)


def solution(mesh):
    return jax.shard_map(
        functools.partial(body, mesh.shape["tmpl"], mesh.shape["grid"]),
        mesh=mesh,
        in_specs=(P("tmpl", "grid", None, None),),
        out_specs=(P(None, "grid", "tmpl", None), P("grid", "tmpl", None)),
        check_vma=False,
    )
```

```python
import functools
import math

import jax
import jax.numpy as jnp
from jax import lax
from jax.experimental import pallas as pl
from jax.experimental.pallas import tpu as pltpu
from jax.sharding import PartitionSpec as P

TOP = 4
KEPT = TOP + 1
SPREAD_FLOOR = 0.25
CHUNKS = 8
HALVED = 4
STEP = 8
TILE = 8
MB = 256
MESH = pl.DeviceIdType.MESH


def fill_table(table):
    doubled = table.shape[0] // 2
    points = doubled // 2
    shape = (doubled, doubled)
    row = lax.broadcasted_iota(jnp.int32, shape, 0)
    lane = lax.broadcasted_iota(jnp.int32, shape, 1)
    turns = (row % points) * (lane % points) + (row // points) * (points // 4)
    turns = (turns + points // 2) % points - points // 2
    phase = jnp.cos(turns.astype(jnp.float32) * (2.0 * math.pi / points))
    lead = phase.astype(jnp.bfloat16).astype(jnp.float32)
    for side in range(2):
        inside = (lane // points) == side
        rows = pl.ds(side * doubled, doubled)
        table[rows, :doubled] = jnp.where(inside, lead, 0.0).astype(jnp.bfloat16)
        table[rows, doubled:] = jnp.where(inside, phase - lead, 0.0).astype(jnp.bfloat16)


def order_pair(former, latter):
    return jnp.maximum(former, latter), jnp.minimum(former, latter)


def order_four(values):
    a, b = order_pair(values[0], values[1])
    c, d = order_pair(values[2], values[3])
    a, c = order_pair(a, c)
    b, d = order_pair(b, d)
    b, c = order_pair(b, c)
    return [a, b, c, d]


def merge_four(former, latter):
    a, b, c, d = (jnp.maximum(former[i], latter[TOP - 1 - i]) for i in range(TOP))
    a, c = order_pair(a, c)
    b, d = order_pair(b, d)
    a, b = order_pair(a, b)
    c, d = order_pair(c, d)
    return [a, b, c, d]


def merge_groups(former, latter):
    return merge_four(former[:TOP], latter[:TOP]) + [former[TOP] + latter[TOP]]


def bits_of(chips):
    return chips.bit_length() - 1


def bit_order(chips, chunk):
    bits = bits_of(chips)
    return [(chunk + phase) % bits for phase in range(bits)]


def shuffled(chips, chunk, chip):
    place = 0
    for bit in bit_order(chips, chunk):
        place = place * 2 + (chip >> bit) % 2
    return place


def kernel(groups, slabs, parts, chunks, spectrum_ref, packed_ref, *scratch):
    local_tmpl, slab_rows, beta_rows, doubled = spectrum_ref.shape
    points = doubled // 2
    half = slab_rows // 2
    chips = groups // 2
    bits = bits_of(chips)
    piece = beta_rows // groups
    per_chunk = half // chunks
    cell_count = float(points * points * points)
    scratch = list(scratch)
    take = scratch.pop
    held, table, score, stats, sent, gathered, average, scale, leaders, sibling, extra, told = (take(0) for _ in range(12))
    work = [take(0) for _ in range(max(bits, 1))]
    arrived = [take(0) for _ in range(bits)]
    landed = take(0)
    halved = min(HALVED, chunks // 2)
    (
        held_sem, stats_send, stats_recv, told_send, told_recv, raw_send, raw_recv,
        pair_send, pair_recv, half_send, half_recv, far_send, far_recv,
    ) = scratch
    count = len(parts) - 1
    late = parts[count - 1]
    late_size = local_tmpl - late
    aligned = piece % TILE == 0

    place = lax.axis_index("tmpl")
    slab = lax.axis_index("grid")
    chip, core = place // 2, place % 2

    def fetch(number):
        return pltpu.make_async_copy(
            spectrum_ref.at[pl.ds(number * STEP, STEP)],
            held.at[pl.ds(number * STEP, STEP)],
            held_sem.at[number],
        )

    for number in range(local_tmpl // STEP):
        fetch(number).start(priority=1)

    def own_bit(bit):
        return (chip // 2**bit) % 2

    partner = (2 * chip + 1 - core, slab)
    across = [(2 * (chip + 2**bit * (1 - 2 * own_bit(bit))) + core, slab) for bit in range(bits)]
    far = [(2 * ((chip + step) % chips) + core, slab) for step in range(1, chips)]
    near = [(place, (slab + step) % slabs) for step in range(1, slabs)]
    beside = [(2 * chip + 1 - core, (slab + step) % slabs) for step in range(slabs)]
    barrier = pltpu.get_barrier_semaphore()
    for device in far + near + beside:
        pl.semaphore_signal(barrier, inc=1, device_id=device, device_id_type=MESH)

    fill_table(table)

    def transform(number, carry):
        fetch(number).wait()
        base = number * STEP
        lines = MB // beta_rows
        for index in range(STEP):
            plain = square = None
            for block in range(half // lines):
                leads, rests = [], []
                for side in range(2):
                    coeffs = held[base + index, pl.ds(side * half + block * lines, lines)].reshape(MB, doubled)
                    lead = coeffs.astype(jnp.bfloat16)
                    leads.append(lead)
                    rests.append((coeffs - lead.astype(jnp.float32)).astype(jnp.bfloat16))
                both = jnp.dot(jnp.concatenate(leads, axis=1), table[...], preferred_element_type=jnp.float32)
                value = both[:, :doubled] + both[:, doubled:] + jnp.dot(jnp.concatenate(rests, axis=1), table[:, :doubled], preferred_element_type=jnp.float32)
                score[base + index, pl.ds(block * lines, lines)] = value.reshape(lines, beta_rows, doubled)
                one = value.reshape(MB // 8, 8, doubled)
                p = jnp.sum(one, axis=0)
                q = jnp.sum(one * one, axis=0)
                plain = p if plain is None else plain + p
                square = q if square is None else square + q
            stats[0, pl.ds(base + index, 1)] = jnp.sum(plain, axis=0, keepdims=True)
            stats[1, pl.ds(base + index, 1)] = jnp.sum(square, axis=0, keepdims=True)
        return carry

    def slots(part):
        tiles = (parts[part + 1] - parts[part]) // TILE
        width = doubled // (2 * tiles)
        lane = lax.broadcasted_iota(jnp.int32, (TILE, doubled), 1)
        places = [(kind, tile) for tile in range(tiles) for kind in range(2)]
        return [
            (kind, parts[part] + tile * TILE, (lane >= index * width) & (lane < (index + 1) * width), width)
            for index, (kind, tile) in enumerate(places)
        ]

    def share_stats(part):
        return [
            pltpu.make_async_remote_copy(
                src_ref=sent.at[part],
                dst_ref=gathered.at[part, step],
                send_sem=stats_send.at[part, step],
                recv_sem=stats_recv.at[part, step],
                device_id=near[step],
                device_id_type=MESH,
            )
            for step in range(slabs - 1)
        ]

    def publish(part):
        message = jnp.zeros((TILE, doubled), jnp.float32)
        for kind, row, mask, _ in slots(part):
            total = jnp.sum(stats[kind, pl.ds(row, TILE)], axis=-1, keepdims=True)
            message = jnp.where(mask, total, message)
        sent[part] = message
        for copy in share_stats(part):
            copy.start()

    def tell_late():
        return [
            pltpu.make_async_remote_copy(
                src_ref=sent.at[count - 1],
                dst_ref=told.at[step],
                send_sem=told_send.at[step],
                recv_sem=told_recv.at[step],
                device_id=beside[step],
                device_id_type=MESH,
            )
            for step in range(slabs)
        ]

    def raw(number, owner):
        base = number * STEP
        spans = [(pair * 2 * piece + owner * piece, piece) for pair in range(chips)] if aligned else [(0, beta_rows)]
        return [
            pltpu.make_async_remote_copy(
                src_ref=score.at[pl.ds(base, STEP), :, pl.ds(pl.multiple_of(start, TILE), size)],
                dst_ref=extra.at[pl.ds(base - late, STEP), :, pl.ds(pl.multiple_of(start, TILE), size)],
                send_sem=raw_send.at[number - late // STEP, index],
                recv_sem=raw_recv.at[number - late // STEP, index],
                device_id=partner,
                device_id_type=MESH,
            )
            for index, (start, size) in enumerate(spans)
        ]

    def spread_out(part, total, shift):
        mean = None
        for kind, row, mask, width in slots(part):
            value = jnp.sum(jnp.where(mask, total, 0.0), axis=-1, keepdims=True) * (1.0 / (width * cell_count))
            if kind == 0:
                mean = value
                continue
            factor = 1.0 / jnp.sqrt(value - mean * mean + SPREAD_FLOOR)
            average[pl.ds(row + shift, TILE)] = jnp.broadcast_to(mean, (TILE, doubled))
            scale[pl.ds(row + shift, TILE)] = jnp.broadcast_to(factor, (TILE, doubled))

    def settle(part):
        for copy in share_stats(part):
            copy.wait_recv()
        if part == count - 1:
            for copy in tell_late():
                copy.wait_recv()
        total = sent[part]
        for step in range(slabs - 1):
            total = total + gathered[part, step]
        if part == count - 1:
            spread_out(part, sum((told[step] for step in range(1, slabs)), told[0]), late_size)
        spread_out(part, total, 0)

    def gather_up(running, values):
        summed = (values[0] + values[1]) + (values[2] + values[3])
        fresh = order_four(values) + [summed]
        return fresh if running is None else merge_groups(running, fresh)

    def last_leading(chunk):
        for row in range(per_chunk):
            line = chunk * per_chunk + row
            for pair in range(chips):
                start = pl.multiple_of(pair * 2 * piece + core * piece, piece)
                window = pl.ds(start, piece)
                running = None
                for base in range(late, local_tmpl, TOP):
                    running = gather_up(running, [
                        (score[tmpl, line, window] - average[pl.ds(tmpl, 1)]) * scale[pl.ds(tmpl, 1)]
                        for tmpl in range(base, base + TOP)
                    ])
                for base in range(0, late_size, TOP):
                    running = gather_up(running, [
                        (extra[tmpl, line, window] - average[pl.ds(local_tmpl + tmpl, 1)]) * scale[pl.ds(local_tmpl + tmpl, 1)]
                        for tmpl in range(base, base + TOP)
                    ])
                former = [leaders[chunk, core, pair, rank, row] for rank in range(KEPT)]
                latter = [sibling[chunk, pair, rank, row] for rank in range(KEPT)]
                running = merge_groups(running, merge_groups(former, latter))
                slot = shuffled(chips, chunk, pair) if chunk < halved else pair
                for rank in range(KEPT):
                    work[0][chunk, slot, rank, row] = running[rank]
        for copy in [halving(0, chunk)] if chunk < halved else scatter(chunk):
            copy.start()

    def leading(part, chunk):
        low, high = parts[part], parts[part + 1]

        def one_row(row, carry):
            line = chunk * per_chunk + row
            for pair in range(chips):
                window = pl.ds(pair * 2 * piece, 2 * piece)
                running = None
                for base in range(low, high, TOP):
                    running = gather_up(running, [
                        (score[tmpl, line, window] - average[pl.ds(tmpl, 1)]) * scale[pl.ds(tmpl, 1)]
                        for tmpl in range(base, base + TOP)
                    ])
                for side in range(2):
                    rows = slice(side * piece, (side + 1) * piece)
                    mine = [value[rows] for value in running]
                    if part > 0:
                        former = [leaders[chunk, side, pair, rank, row] for rank in range(KEPT)]
                        mine = merge_groups(former, mine)
                    for rank in range(KEPT):
                        leaders[chunk, side, pair, rank, row] = mine[rank]
            return carry

        lax.fori_loop(0, per_chunk, one_row, 0)

    def exchange(chunk):
        return pltpu.make_async_remote_copy(
            src_ref=leaders.at[chunk, 1 - core],
            dst_ref=sibling.at[chunk],
            send_sem=pair_send.at[chunk],
            recv_sem=pair_recv.at[chunk],
            device_id=partner,
            device_id_type=MESH,
        )

    def halving(phase, chunk):
        bit = bit_order(chips, chunk)[phase]
        kept = chips >> (phase + 1)
        return pltpu.make_async_remote_copy(
            src_ref=work[phase].at[chunk, pl.ds((1 - own_bit(bit)) * kept, kept)],
            dst_ref=arrived[phase].at[chunk],
            send_sem=half_send.at[phase, chunk],
            recv_sem=half_recv.at[phase, chunk],
            device_id=across[bit],
            device_id_type=MESH,
        )

    def scatter(chunk):
        return [
            pltpu.make_async_remote_copy(
                src_ref=work[0].at[chunk, (chip + step) % chips],
                dst_ref=landed.at[chunk - halved, step - 1],
                send_sem=far_send.at[chunk - halved, step - 1],
                recv_sem=far_recv.at[chunk - halved, step - 1],
                device_id=far[step - 1],
                device_id_type=MESH,
            )
            for step in range(1, chips)
        ]

    def join_scattered(chunk):
        for copy in scatter(chunk):
            copy.wait_recv()
        for row in range(per_chunk):
            running = [work[0][chunk, chip, rank, row] for rank in range(KEPT)]
            for step in range(chips - 1):
                running = merge_groups(running, [landed[chunk - halved, step, rank, row] for rank in range(KEPT)])
            hand_on(bits, chunk, 0, running, row)

    def hand_on(phase, chunk, slot, values, row):
        if phase < bits:
            for rank in range(KEPT):
                work[phase][chunk, slot, rank, row] = values[rank]
            return
        values[TOP] = values[TOP] / math.sqrt(groups * local_tmpl)
        for rank in range(KEPT):
            packed_ref[rank, chunk * per_chunk + row] = values[rank]

    def join_far(phase, chunk):
        halving(phase, chunk).wait_recv()
        kept = chips >> (phase + 1)
        mine = own_bit(bit_order(chips, chunk)[phase]) * kept
        for slot in range(kept):
            for row in range(per_chunk):
                former = [work[phase][chunk, mine + slot, rank, row] for rank in range(KEPT)]
                latter = [arrived[phase][chunk, slot, rank, row] for rank in range(KEPT)]
                hand_on(phase + 1, chunk, slot, merge_groups(former, latter), row)
        if phase + 1 < bits:
            halving(phase + 1, chunk).start()

    late_numbers = range(late // STEP, local_tmpl // STEP)
    for part in range(count - 1):
        lax.fori_loop(parts[part] // STEP, parts[part + 1] // STEP, transform, 0)
        if part == 0:
            pl.semaphore_wait(barrier, len(far) + len(near) + len(beside))
        publish(part)
    for number in late_numbers:
        transform(number, 0)
    publish(count - 1)
    for copy in tell_late():
        copy.start()
    for number in late_numbers:
        for copy in raw(number, 1 - core):
            copy.start()
    for part in range(count - 1):
        settle(part)
        for chunk in range(chunks):
            leading(part, chunk)
            if part == count - 2:
                exchange(chunk).start()
    for number in late_numbers:
        for copy in raw(number, core):
            copy.wait_recv()
    for chunk in range(chunks):
        exchange(chunk).wait_recv()
    settle(count - 1)
    for chunk in range(chunks):
        last_leading(chunk)
    for part in range(count):
        for copy in share_stats(part):
            copy.wait_send()
    for copy in tell_late():
        copy.wait_send()
    for number in late_numbers:
        for copy in raw(number, 1 - core):
            copy.wait_send()
    for chunk in range(chunks):
        exchange(chunk).wait_send()
    for chunk in range(halved):
        join_far(0, chunk)
    for chunk in range(halved):
        halving(0, chunk).wait_send()
    for chunk in range(halved, chunks):
        join_scattered(chunk)
    for phase in range(1, bits):
        for chunk in range(halved):
            join_far(phase, chunk)
    for chunk in range(halved, chunks):
        for copy in scatter(chunk):
            copy.wait_send()
    for phase in range(1, bits):
        for chunk in range(halved):
            halving(phase, chunk).wait_send()


def unpack(packed_ref, best_ref, coherence_ref):
    half, points = packed_ref.shape[1], best_ref.shape[-1]
    for side in range(2):
        rows = pl.ds(side * half, half)
        lanes = slice(side * points, (side + 1) * points)
        best_ref[:, rows] = packed_ref[:TOP, :, :, lanes]
        coherence_ref[rows] = packed_ref[TOP, :, :, lanes]


def body(groups, slabs, spectrum):
    local_tmpl, slab_rows, beta_rows, doubled = spectrum.shape
    points = doubled // 2
    half = slab_rows // 2
    chips = groups // 2
    bits = bits_of(chips)
    piece = beta_rows // groups
    chunks = min(CHUNKS, half)
    halved = min(HALVED, chunks // 2)
    per_chunk = half // chunks
    parts = (0, local_tmpl // 2, local_tmpl)
    late_size = parts[-1] - parts[-2]
    spans = chips if piece % TILE == 0 else 1
    count = len(parts) - 1
    block = (KEPT, per_chunk, piece, doubled)
    f32 = jnp.float32
    dma = pltpu.SemaphoreType.DMA
    packed = pl.pallas_call(
        functools.partial(kernel, groups, slabs, parts, chunks),
        out_shape=jax.ShapeDtypeStruct((KEPT, half, piece, doubled), f32),
        in_specs=[pl.BlockSpec(memory_space=pltpu.HBM)],
        out_specs=pl.BlockSpec(memory_space=pltpu.VMEM),
        scratch_shapes=[
            pltpu.VMEM((local_tmpl, slab_rows, beta_rows, doubled), f32),
            pltpu.VMEM((2 * doubled, 2 * doubled), jnp.bfloat16),
            pltpu.VMEM((local_tmpl, half, beta_rows, doubled), f32),
            pltpu.VMEM((2, local_tmpl, doubled), f32),
            pltpu.VMEM((count, TILE, doubled), f32),
            pltpu.VMEM((count, slabs - 1, TILE, doubled), f32),
            pltpu.VMEM((local_tmpl + late_size, doubled), f32),
            pltpu.VMEM((local_tmpl + late_size, doubled), f32),
            pltpu.VMEM((chunks, 2, chips) + block, f32),
            pltpu.VMEM((chunks, chips) + block, f32),
            pltpu.VMEM((late_size, half, beta_rows, doubled), f32),
            pltpu.VMEM((slabs, TILE, doubled), f32),
        ]
        + [pltpu.VMEM((chunks, chips >> phase) + block, f32) for phase in range(max(bits, 1))]
        + [pltpu.VMEM((chunks, chips >> (phase + 1)) + block, f32) for phase in range(bits)]
        + [pltpu.VMEM((chunks - halved, chips - 1) + block, f32)]
        + [
            dma((local_tmpl // STEP,)),
            dma((count, slabs - 1)),
            dma((count, slabs - 1)),
            dma((slabs,)),
            dma((slabs,)),
            dma((late_size // STEP, spans)),
            dma((late_size // STEP, spans)),
            dma((chunks,)),
            dma((chunks,)),
            dma((bits, chunks)),
            dma((bits, chunks)),
            dma((chunks - halved, chips - 1)),
            dma((chunks - halved, chips - 1)),
        ],
        compiler_params=pltpu.CompilerParams(
            collective_id=0, has_side_effects=True, vmem_limit_bytes=48 * 1024 * 1024
        ),
    )(spectrum)
    return pl.pallas_call(
        unpack,
        out_shape=(
            jax.ShapeDtypeStruct((TOP, slab_rows, piece, points), f32),
            jax.ShapeDtypeStruct((slab_rows, piece, points), f32),
        ),
        compiler_params=pltpu.CompilerParams(vmem_limit_bytes=8 * 1024 * 1024),
    )(packed)


def solution(mesh):
    return jax.shard_map(
        functools.partial(body, mesh.shape["tmpl"], mesh.shape["grid"]),
        mesh=mesh,
        in_specs=(P("tmpl", "grid", None, None),),
        out_specs=(P(None, "grid", "tmpl", None), P("grid", "tmpl", None)),
        check_vma=False,
    )
```
